256 devices in a mesh: seq: 64 (over x, z, core), head: 4 (over y).
Axes of the slice: x: 4, y: 4, z: 8, core: 2. Of those that a mesh axis runs over, the one named last changes fastest.
Arguments:
- queries: bfloat16 [32768, 4096], P('seq', 'head'), may hold values from -120 to 120
- keys: bfloat16 [32768, 1024], P('seq', 'head'), may hold values from -4 to 4
- values: bfloat16 [32768, 1024], P('seq', 'head'), may hold values from -6 to 6
- doc_start: int32 [32768], P('seq'), may hold values from 0 to 32767, as said below
- hop_counts: int32 [64], P('seq'), may hold values from 0 to 4, as said below
- loss_mask: int32 [32768], P('seq'), may hold values from 0 to 1, as said below
Outputs:
- attention: bfloat16 [32768, 4096], P('seq', 'head')
- objective: float32 [], replicated
The draws below stay inside these ranges and needn't reach their ends.
Inputs may be any that keep to these rules, and one draw needn't show every extreme that they name: doc_start is nondecreasing; doc_start[doc_start[i]] = doc_start[i] <= i; a document holds at most 2048 tokens, and some document holds exactly that many in every draw. hop_counts[b] = b - floor(doc_start[b * 512] / 512); the most, 4, is reached in every draw. loss_mask[0] = 1.
All inputs are finite; a program needn't handle non-finite values.
Results may differ from the reference program's by a relative error of at most 0.0035.
Values may be sent and summed in bfloat16 or wider, within the bound.
A program may use at most 128 MiB of HBM per device.

```python
import math
import jax
import jax.numpy as jnp
from jax import lax

QUERY_HEADS = 32
KEY_VALUE_HEADS = 8
HEAD_WIDTH = 128
BLOCK_TOKENS = 512
HOPS = 4
PACKED_TOKENS = 32768


def doc_layout(key):
    span = HOPS * BLOCK_TOKENS
    places = jnp.arange(PACKED_TOKENS, dtype=jnp.int32)
    windows = PACKED_TOKENS // span + 2
    rates = jax.random.randint(jax.random.fold_in(key, 11), (windows,), 0, 3)
    levels = jnp.array([2, 4, 8], dtype=jnp.int32)[rates]
    whole_window = jax.random.randint(jax.random.fold_in(key, 13), (), 0, max(PACKED_TOKENS // span - 1, 1))
    window_ids = jnp.arange(windows, dtype=jnp.int32)
    levels = jnp.where(window_ids == whole_window, 0, levels)
    ticket = jax.random.randint(jax.random.fold_in(key, 12), (PACKED_TOKENS,), 0, span)
    window_of = jnp.maximum(places - 1, 0) // span
    flagged = (places % span == 1) | (places == 0) | (places == PACKED_TOKENS - 1) | (ticket < levels[window_of])
    starts = lax.cummax(jnp.where(flagged, places, 0), axis=0)
    block_ids = jnp.arange(PACKED_TOKENS // BLOCK_TOKENS, dtype=jnp.int32)
    hops = block_ids - starts[block_ids * BLOCK_TOKENS] // BLOCK_TOKENS
    return (starts.astype(jnp.int32), hops.astype(jnp.int32))


def draw_doc_start(key, part):
    return doc_layout(key)[0]


def draw_hop_counts(key, part):
    return doc_layout(key)[1]


def draw_loss_mask(key, part):
    places = jnp.arange(PACKED_TOKENS, dtype=jnp.int32)
    ticket = jax.random.randint(jax.random.fold_in(key, 31), (PACKED_TOKENS,), 0, 1000)
    marks = (ticket < 200 + 500 * places // PACKED_TOKENS).astype(jnp.int32)
    return marks.at[0].set(1)


def query_keys(key):
    resident_keys = jnp.clip(jax.random.normal(jax.random.fold_in(key, 21), (PACKED_TOKENS, KEY_VALUE_HEADS * HEAD_WIDTH), jnp.float32), -4.0, 4.0)
    base_queries = jnp.clip(jax.random.normal(jax.random.fold_in(key, 22), (PACKED_TOKENS, QUERY_HEADS * HEAD_WIDTH), jnp.float32), -4.0, 4.0)
    return (base_queries, resident_keys)


def draw_queries(key, part):
    return query_keys(key)[0].astype(jnp.bfloat16)


def draw_keys(key, part):
    return query_keys(key)[1].astype(jnp.bfloat16)


def block_levels(rng, shape, pieces, low, top_value):
    level = 1.0
    for dim, shards_of in pieces:
        steps = jax.random.uniform(jax.random.fold_in(jax.random.fold_in(rng, 6), dim), (shards_of,), jnp.float32, low / len(pieces), top_value / len(pieces))
        level = level * jnp.repeat(jnp.exp(steps), shape[dim] // shards_of).reshape((-1,) + (1,) * (len(shape) - 1 - dim))
    return level


def centred(stream_key, extent, scale, reach, pieces=(), kind=jnp.bfloat16):
    level = block_levels(stream_key, extent, pieces, -0.22, 0.18) if pieces else 1.0
    result = jax.random.normal(stream_key, extent, jnp.float32) * scale * level
    return jnp.minimum(jnp.maximum(result, -reach), reach).astype(kind)


def setup_inputs(seed: int = 0) -> dict:
    arg_keys = jax.random.split(jax.random.key(seed), 7)
    queries = draw_queries(jax.random.fold_in(arg_keys[6], 71), 0)
    keys = draw_keys(jax.random.fold_in(arg_keys[6], 71), 0)
    values = centred(arg_keys[2], (PACKED_TOKENS, KEY_VALUE_HEADS * HEAD_WIDTH), 1.0, 6.0, ((0, 64), (1, 4)))
    doc_start = draw_doc_start(jax.random.fold_in(arg_keys[6], 71), 0)
    hop_counts = draw_hop_counts(jax.random.fold_in(arg_keys[6], 71), 0)
    loss_mask = draw_loss_mask(jax.random.fold_in(arg_keys[6], 71), 0)
    return {"queries": queries, "keys": keys, "values": values, "doc_start": doc_start, "hop_counts": hop_counts, "loss_mask": loss_mask}


def reference(queries, keys, values, doc_start, hop_counts, loss_mask):
    group_size = QUERY_HEADS // KEY_VALUE_HEADS
    blocks = PACKED_TOKENS // BLOCK_TOKENS
    border_width = HOPS * BLOCK_TOKENS
    reach_extent = (HOPS + 1) * BLOCK_TOKENS
    key_padding = jnp.concatenate([jnp.zeros((border_width, KEY_VALUE_HEADS * HEAD_WIDTH), keys.dtype), keys], axis=0)
    value_padding = jnp.concatenate([jnp.zeros((border_width, KEY_VALUE_HEADS * HEAD_WIDTH), values.dtype), values], axis=0)

    def one_block(block):
        block_offset = (block * BLOCK_TOKENS).astype(jnp.int32)
        query_row_block = lax.dynamic_slice_in_dim(queries, block_offset, BLOCK_TOKENS, 0).reshape(BLOCK_TOKENS, KEY_VALUE_HEADS, group_size, HEAD_WIDTH).astype(jnp.float32)
        key_row_block = lax.dynamic_slice_in_dim(key_padding, block_offset, reach_extent, 0).reshape(reach_extent, KEY_VALUE_HEADS, HEAD_WIDTH).astype(jnp.float32)
        value_row_block = lax.dynamic_slice_in_dim(value_padding, block_offset, reach_extent, 0).reshape(reach_extent, KEY_VALUE_HEADS, HEAD_WIDTH).astype(jnp.float32)
        scores = jnp.einsum('tgqd,sgd->tgqs', query_row_block, key_row_block) / math.sqrt(HEAD_WIDTH)
        key_place = block_offset - border_width + jnp.arange(reach_extent, dtype=jnp.int32)
        query_place = block_offset + jnp.arange(BLOCK_TOKENS, dtype=jnp.int32)
        firsts = lax.dynamic_slice_in_dim(doc_start, block_offset, BLOCK_TOKENS, 0)
        hop_limit = lax.dynamic_index_in_dim(hop_counts, block, 0, keepdims=False)
        distance = block - jnp.floor_divide(key_place, BLOCK_TOKENS)
        seen = (key_place[None, :] >= firsts[:, None]) & (key_place[None, :] <= query_place[:, None]) & (distance <= hop_limit)[None, :]
        seen = seen[:, None, None, :]
        masked = jnp.where(seen, scores, jnp.float32(-1e+30))
        top = lax.optimization_barrier(jnp.max(masked, axis=-1, keepdims=True))
        weights = jnp.where(seen, jnp.exp(masked - top), jnp.float32(0.0))
        total = lax.optimization_barrier(jnp.sum(weights, axis=-1))
        rounded = lax.optimization_barrier(weights.astype(jnp.bfloat16))
        numer = jnp.einsum('tgqs,sgd->tgqd', rounded.astype(jnp.float32), value_row_block)
        attended = (numer / total[..., None]).reshape(BLOCK_TOKENS, QUERY_HEADS * HEAD_WIDTH)
        marks = lax.dynamic_slice_in_dim(loss_mask, block_offset, BLOCK_TOKENS, 0).astype(jnp.float32)
        squares = jnp.sum(marks[:, None] * attended * attended)
        return (attended.astype(jnp.bfloat16), squares)
    outputs, squares = lax.map(one_block, jnp.arange(blocks, dtype=jnp.int32))
    attention = outputs.reshape(PACKED_TOKENS, QUERY_HEADS * HEAD_WIDTH)
    counted = jnp.sum(loss_mask.astype(jnp.float32))
    objective = jnp.sum(squares) / (QUERY_HEADS * counted)
    return (attention, objective)
```

```python
import functools
import math

import jax
import jax.numpy as jnp
from jax import lax
from jax.experimental import pallas as pl
from jax.experimental.pallas import tpu as pltpu
from jax.sharding import Mesh
from jax.sharding import PartitionSpec as P

QUERY_HEADS = 32
KEY_VALUE_HEADS = 8
HEAD_WIDTH = 128
HOPS = 4
GROUP = QUERY_HEADS // KEY_VALUE_HEADS
CHUNKS = 4
SEQ = ("seq_0", "seq_1", "seq_2")
MESH = pl.DeviceIdType.MESH
EXP_SCALE = math.log2(math.e) / math.sqrt(HEAD_WIDTH)
HIDDEN = -1e30


def kernel(
    sizes,
    q_hbm,
    k_hbm,
    v_hbm,
    doc_ref,
    hop_ref,
    mark_ref,
    out_hbm,
    obj_ref,
    kv,
    q_in,
    q_t,
    acc,
    top,
    total,
    bias,
    out_vm,
    parts_c,
    parts_h,
    parts_x,
    parts_z,
    load_sem,
    store_sem,
    send_sem,
    recv_sem,
    part_send,
    part_recv,
):
    nx, nz, nc, nh = sizes
    rows = q_in.shape[0]
    kv_heads = kv.shape[3] // HEAD_WIDTH
    heads = kv_heads * GROUP
    step_rows = rows // CHUNKS
    ix, iz, ic, ih = (lax.axis_index(a) for a in (*SEQ, "head"))
    chip = ix * nz + iz
    block = chip * nc + ic
    after = lax.rem(chip + 1, nx * nz)
    before = lax.rem(chip + nx * nz - 1, nx * nz)
    next_chip = {"seq_0": after // nz, "seq_1": lax.rem(after, nz)}
    last_chip = {"seq_0": before // nz, "seq_1": lax.rem(before, nz)}
    partner = {"seq_2": 1 - ic}
    axes = (("seq_2", nc, ic), ("head", nh, ih), ("seq_0", nx, ix), ("seq_1", nz, iz))

    loads = (
        pltpu.make_async_copy(k_hbm, kv.at[0, 0], load_sem.at[0]),
        pltpu.make_async_copy(v_hbm, kv.at[0, 1], load_sem.at[1]),
        pltpu.make_async_copy(q_hbm, q_in, load_sem.at[2]),
    )
    for load in loads:
        load.start()

    barrier = pltpu.get_barrier_semaphore()
    signals = 2
    pl.semaphore_signal(barrier, inc=1, device_id=next_chip, device_id_type=MESH)
    pl.semaphore_signal(barrier, inc=1, device_id=last_chip, device_id_type=MESH)
    for name, size, here in axes:
        for d in range(1, size):
            pl.semaphore_signal(
                barrier, inc=1, device_id={name: lax.rem(here + d, size)}, device_id_type=MESH
            )
            signals += 1
    loads[0].wait()
    loads[1].wait()
    pl.semaphore_wait(barrier, signals)

    def piece(slot, c):
        return kv.at[slot, :, pl.ds(pl.multiple_of(c * step_rows, step_rows), step_rows), :]

    def hand_on(kind, slot, c, to_slot, device):
        return pltpu.make_async_remote_copy(
            src_ref=piece(slot, c),
            dst_ref=piece(to_slot, c),
            send_sem=send_sem.at[kind, c],
            recv_sem=recv_sem.at[to_slot, c],
            device_id=device,
            device_id_type=MESH,
        )

    def arrived(slot, c):
        hand_on(0, 0, c, slot, next_chip).wait_recv()

    for c in range(CHUNKS):
        hand_on(0, 0, c, 2, next_chip).start()

    @pl.when(ic == 0)
    def _():
        for c in range(CHUNKS):
            hand_on(2, 0, c, 1, partner).start()

    loads[2].wait()
    for h in range(heads):
        q_t[h] = q_in[:, h * HEAD_WIDTH : (h + 1) * HEAD_WIDTH].T
    top[...] = jnp.full(top.shape, HIDDEN, jnp.float32)
    total[...] = jnp.zeros(total.shape, jnp.float32)
    acc[...] = jnp.zeros(acc.shape, jnp.float32)

    first_key = jnp.maximum(doc_ref[...], (block - hop_ref[0]) * rows)
    q_place = block * rows + lax.broadcasted_iota(jnp.int32, (1, rows), 1)

    def attend(slot_a, c_a, slot_b, c_b):
        at_a = pl.ds(pl.multiple_of(c_a * step_rows, step_rows), step_rows)
        at_b = pl.ds(pl.multiple_of(c_b * step_rows, step_rows), step_rows)
        inside = lax.broadcasted_iota(jnp.int32, (step_rows, rows), 0)
        for i, (slot, c) in enumerate(((slot_a, c_a), (slot_b, c_b))):
            place = inside + ((block - slot) * rows + c * step_rows)
            seen = (place >= first_key) & (place <= q_place)
            bias[i * step_rows : (i + 1) * step_rows, :] = jnp.where(seen, 0.0, HIDDEN)
        for g in range(kv_heads):
            lanes = slice(g * HEAD_WIDTH, (g + 1) * HEAD_WIDTH)
            k_two = jnp.concatenate([kv[slot_a, 0, at_a, lanes], kv[slot_b, 0, at_b, lanes]], 0)
            v_two = jnp.concatenate([kv[slot_a, 1, at_a, lanes], kv[slot_b, 1, at_b, lanes]], 0)
            v_t = v_two.T
            for h in range(g * GROUP, (g + 1) * GROUP):
                scores = jnp.dot(k_two, q_t[h], preferred_element_type=jnp.float32) + bias[...]
                old = top[h : h + 1, :]
                new = jnp.maximum(old, jnp.max(scores, axis=0, keepdims=True))
                weights = jnp.exp2((scores - new) * EXP_SCALE)
                ratio = jnp.exp2((old - new) * EXP_SCALE)
                total[h : h + 1, :] = total[h : h + 1, :] * ratio + jnp.sum(
                    weights, axis=0, keepdims=True
                )
                update = jnp.dot(
                    v_t, weights.astype(jnp.bfloat16), preferred_element_type=jnp.float32
                )
                acc[h] = acc[h] * ratio + update
                top[h : h + 1, :] = new

    def own(i, _):
        attend(0, 2 * i, 0, 2 * i + 1)
        return 0

    lax.fori_loop(0, CHUNKS // 2, own, 0)

    def neighbour(i, _):
        arrived(1, 2 * i)
        arrived(1, 2 * i + 1)
        attend(1, 2 * i, 1, 2 * i + 1)
        return 0

    lax.fori_loop(0, jnp.where(ic == 1, CHUNKS // 2, 0), neighbour, 0)

    mixed = jnp.where(ic == 0, 1, 3)

    def middle(c, _):
        arrived(2, c)
        hand_on(1, 2, c, 4, next_chip).start()
        hand_on(3, 2, c, 4 - mixed, partner).start()
        arrived(mixed, c)
        attend(2, c, mixed, c)
        return 0

    lax.fori_loop(0, CHUNKS, middle, 0)

    @pl.when(ic == 0)
    def _():
        def far(c, _):
            arrived(4, c)
            arrived(3, c)
            attend(4, c, 3, c)
            return 0

        lax.fori_loop(0, CHUNKS, far, 0)

    @pl.when(ic == 1)
    def _():
        def far(i, _):
            for c in (2 * i, 2 * i + 1):
                arrived(4, c)
                hand_on(4, 4, c, 3, partner).start()
            attend(4, 2 * i, 4, 2 * i + 1)
            return 0

        lax.fori_loop(0, CHUNKS // 2, far, 0)

    marks = mark_ref[...].astype(jnp.float32)
    squares = jnp.zeros((1, rows), jnp.float32)
    for h in range(heads):
        attended = acc[h] * (1.0 / total[h : h + 1, :])
        squares = squares + jnp.sum(attended * attended, axis=0, keepdims=True)
        out_vm[:, h * HEAD_WIDTH : (h + 1) * HEAD_WIDTH] = attended.astype(jnp.bfloat16).T
    store = pltpu.make_async_copy(out_vm, out_hbm, store_sem)
    store.start()

    def folded(row):
        return sum(row[:, i : i + 128] for i in range(0, rows, 128))

    part = jnp.concatenate([folded(marks * squares), folded(marks)], 0)
    sent = []
    for stage, ((name, size, here), parts) in enumerate(
        zip(axes, (parts_c, parts_h, parts_x, parts_z), strict=True)
    ):
        parts[here] = part
        copies = []
        for d in range(1, size):
            peer = lax.rem(here + d, size)
            copy = pltpu.make_async_remote_copy(
                src_ref=parts.at[here],
                dst_ref=parts.at[here],
                send_sem=part_send.at[stage, d],
                recv_sem=part_recv.at[stage, here],
                device_id={name: peer},
                device_id_type=MESH,
            )
            copy.start()
            copies.append(copy)
        for d in range(1, size):
            peer = lax.rem(here + d, size)
            pltpu.make_async_remote_copy(
                src_ref=parts.at[here],
                dst_ref=parts.at[peer],
                send_sem=part_send.at[stage, d],
                recv_sem=part_recv.at[stage, peer],
                device_id={name: peer},
                device_id_type=MESH,
            ).wait_recv()
        part = parts[0]
        for i in range(1, size):
            part = part + parts[i]
        sent += copies
    objective = jnp.sum(part[0:1, :]) / ((QUERY_HEADS // nh) * jnp.sum(part[1:2, :]))
    obj_ref[0, 0] = objective

    for copy in sent:
        copy.wait_send()
    for c in range(CHUNKS):
        hand_on(0, 0, c, 2, next_chip).wait_send()
        hand_on(1, 2, c, 4, next_chip).wait_send()
        hand_on(3, 2, c, 4 - mixed, partner).wait_send()

    @pl.when(ic == 0)
    def _():
        for c in range(CHUNKS):
            hand_on(2, 0, c, 1, partner).wait_send()

    @pl.when(ic == 1)
    def _():
        for c in range(CHUNKS):
            hand_on(4, 4, c, 3, partner).wait_send()

    store.wait()


def on_device(sizes, queries, keys, values, doc_start, hop_counts, loss_mask):
    nx, nz, nc, nh = sizes
    rows, width = queries.shape
    kv_width = keys.shape[1]
    heads = width // HEAD_WIDTH
    most = max(sizes)
    attention, objective = pl.pallas_call(
        functools.partial(kernel, sizes),
        out_shape=(
            jax.ShapeDtypeStruct((rows, width), jnp.bfloat16),
            jax.ShapeDtypeStruct((1, 1), jnp.float32),
        ),
        in_specs=[
            pl.BlockSpec(memory_space=pl.ANY),
            pl.BlockSpec(memory_space=pl.ANY),
            pl.BlockSpec(memory_space=pl.ANY),
            pl.BlockSpec(memory_space=pltpu.VMEM),
            pl.BlockSpec(memory_space=pltpu.SMEM),
            pl.BlockSpec(memory_space=pltpu.VMEM),
        ],
        out_specs=(
            pl.BlockSpec(memory_space=pl.ANY),
            pl.BlockSpec(memory_space=pltpu.SMEM),
        ),
        scratch_shapes=[
            pltpu.VMEM((HOPS + 1, 2, rows, kv_width), jnp.bfloat16),
            pltpu.VMEM((rows, width), jnp.bfloat16),
            pltpu.VMEM((heads, HEAD_WIDTH, rows), jnp.bfloat16),
            pltpu.VMEM((heads, HEAD_WIDTH, rows), jnp.float32),
            pltpu.VMEM((heads, rows), jnp.float32),
            pltpu.VMEM((heads, rows), jnp.float32),
            pltpu.VMEM((2 * rows // CHUNKS, rows), jnp.float32),
            pltpu.VMEM((rows, width), jnp.bfloat16),
            pltpu.VMEM((nc, 2, 128), jnp.float32),
            pltpu.VMEM((nh, 2, 128), jnp.float32),
            pltpu.VMEM((nx, 2, 128), jnp.float32),
            pltpu.VMEM((nz, 2, 128), jnp.float32),
            pltpu.SemaphoreType.DMA((3,)),
            pltpu.SemaphoreType.DMA,
            pltpu.SemaphoreType.DMA((5, CHUNKS)),
            pltpu.SemaphoreType.DMA((HOPS + 1, CHUNKS)),
            pltpu.SemaphoreType.DMA((4, most)),
            pltpu.SemaphoreType.DMA((4, most)),
        ],
        compiler_params=pltpu.CompilerParams(collective_id=0, has_side_effects=True),
    )(
        queries,
        keys,
        values,
        doc_start.reshape(1, rows),
        hop_counts,
        loss_mask.reshape(1, rows),
    )
    return attention, objective.reshape(())


def solution(mesh):
    nh = mesh.shape["head"]
    devices = mesh.devices.reshape(4, 8, 2, nh)
    torus = Mesh(devices, (*SEQ, "head"))
    placed = (P(SEQ, "head"), P(SEQ, "head"), P(SEQ, "head"), P(SEQ), P(SEQ), P(SEQ))
    return jax.shard_map(
        functools.partial(on_device, devices.shape),
        mesh=torus,
        in_specs=placed,
        out_specs=(P(SEQ, "head"), P()),
        check_vma=False,
    )
```

```python
import functools
import math

import jax
import jax.numpy as jnp
from jax import lax
from jax.experimental import pallas as pl
from jax.experimental.pallas import tpu as pltpu
from jax.sharding import Mesh
from jax.sharding import PartitionSpec as P

QUERY_HEADS = 32
KEY_VALUE_HEADS = 8
HEAD_WIDTH = 128
HOPS = 4
GROUP = QUERY_HEADS // KEY_VALUE_HEADS
CHUNKS = 4
SEQ = ("seq_0", "seq_1", "seq_2")
MESH = pl.DeviceIdType.MESH
EXP_SCALE = math.log2(math.e) / math.sqrt(HEAD_WIDTH)
HIDDEN = -1e30


def kernel(
    sizes,
    q_hbm,
    k_hbm,
    v_hbm,
    doc_hbm,
    hop_hbm,
    mark_hbm,
    out_hbm,
    obj_ref,
    kv,
    doc_ref,
    hop_ref,
    mark_ref,
    q_in,
    q_t,
    acc,
    top,
    total,
    bias,
    out_vm,
    parts_a,
    parts_b,
    load_sem,
    store_sem,
    send_sem,
    recv_sem,
    part_send,
    part_recv,
    met,
):
    nx, nz, nc, nh = sizes
    rows = q_in.shape[0]
    kv_heads = kv.shape[3] // HEAD_WIDTH
    heads = kv_heads * GROUP
    step_rows = rows // CHUNKS
    ix, iz, ic, ih = (lax.axis_index(a) for a in (*SEQ, "head"))
    chip = ix * nz + iz
    block = chip * nc + ic
    after = lax.rem(chip + 1, nx * nz)
    before = lax.rem(chip + nx * nz - 1, nx * nz)
    next_chip = {"seq_0": after // nz, "seq_1": lax.rem(after, nz)}
    last_chip = {"seq_0": before // nz, "seq_1": lax.rem(before, nz)}
    partner = {"seq_2": 1 - ic}
    planes = (
        (("seq_1", nz, iz), ("seq_2", nc, ic)),
        (("head", nh, ih), ("seq_0", nx, ix)),
    )

    def others(plane):
        (name_a, size_a, here_a), (name_b, size_b, here_b) = plane
        for d in range(1, size_a * size_b):
            at_a = lax.rem(here_a + d // size_b, size_a)
            at_b = lax.rem(here_b + d % size_b, size_b)
            yield d, at_a * size_b + at_b, {name_a: at_a, name_b: at_b}


    loads = (
        pltpu.make_async_copy(k_hbm, kv.at[0, 0], load_sem.at[0]),
        pltpu.make_async_copy(v_hbm, kv.at[0, 1], load_sem.at[1]),
        pltpu.make_async_copy(q_hbm, q_in, load_sem.at[2]),
        pltpu.make_async_copy(doc_hbm, doc_ref, load_sem.at[3]),
        pltpu.make_async_copy(hop_hbm, hop_ref, load_sem.at[4]),
        pltpu.make_async_copy(mark_hbm, mark_ref, load_sem.at[5]),
    )
    for load in loads:
        load.start()

    def along(name, size, here, steps):
        return [{name: lax.rem(here + d, size)} for d in sorted({s % size for s in steps} - {0})]

    def greet(semaphore, devices):
        for device in devices:
            pl.semaphore_signal(semaphore, inc=1, device_id=device, device_id_type=MESH)
        return len(devices)

    one_hop = [
        *along("seq_1", nz, iz, (1, -1)),
        *along("seq_0", nx, ix, (1, -1)),
        *along("head", nh, ih, (1, -1)),
    ]
    barrier = pltpu.get_barrier_semaphore()
    signals = greet(barrier, [next_chip, last_chip, partner, *one_hop])
    loads[0].wait()
    loads[1].wait()
    pl.semaphore_wait(barrier, signals)

    def piece(slot, c):
        return kv.at[slot, :, pl.ds(pl.multiple_of(c * step_rows, step_rows), step_rows), :]

    def hand_on(kind, slot, c, to_slot, device):
        return pltpu.make_async_remote_copy(
            src_ref=piece(slot, c),
            dst_ref=piece(to_slot, c),
            send_sem=send_sem.at[kind, c],
            recv_sem=recv_sem.at[to_slot, c],
            device_id=device,
            device_id_type=MESH,
        )

    def arrived(slot, c):
        hand_on(0, 0, c, slot, next_chip).wait_recv()

    for c in range(CHUNKS):
        hand_on(0, 0, c, 2, next_chip).start()

    @pl.when(ic == 0)
    def _():
        for c in range(CHUNKS):
            hand_on(2, 0, c, 1, partner).start()

    round_one = greet(met.at[0], one_hop)
    for load in loads[2:]:
        load.wait()
    for h in range(heads):
        q_t[h] = q_in[:, h * HEAD_WIDTH : (h + 1) * HEAD_WIDTH].T
    top[...] = jnp.full(top.shape, HIDDEN, jnp.float32)
    total[...] = jnp.zeros(total.shape, jnp.float32)
    acc[...] = jnp.zeros(acc.shape, jnp.float32)

    first_key = jnp.maximum(doc_ref[...], (block - hop_ref[0]) * rows)
    q_place = block * rows + lax.broadcasted_iota(jnp.int32, (1, rows), 1)

    def attend(slot_a, c_a, slot_b, c_b):
        at_a = pl.ds(pl.multiple_of(c_a * step_rows, step_rows), step_rows)
        at_b = pl.ds(pl.multiple_of(c_b * step_rows, step_rows), step_rows)
        inside = lax.broadcasted_iota(jnp.int32, (step_rows, rows), 0)
        for i, (slot, c) in enumerate(((slot_a, c_a), (slot_b, c_b))):
            place = inside + ((block - slot) * rows + c * step_rows)
            seen = (place >= first_key) & (place <= q_place)
            bias[i * step_rows : (i + 1) * step_rows, :] = jnp.where(seen, 0.0, HIDDEN)
        k_two, v_t = [], []
        for g in range(kv_heads):
            lanes = slice(g * HEAD_WIDTH, (g + 1) * HEAD_WIDTH)
            k_two.append(jnp.concatenate([kv[slot_a, 0, at_a, lanes], kv[slot_b, 0, at_b, lanes]], 0))
            v_two = jnp.concatenate([kv[slot_a, 1, at_a, lanes], kv[slot_b, 1, at_b, lanes]], 0)
            v_t.append(v_two.T)

        def score(h):
            return jnp.dot(k_two[h // GROUP], q_t[h], preferred_element_type=jnp.float32) + bias[...]

        def absorb(h, rounded, ratio):
            update = jnp.dot(v_t[h // GROUP], rounded, preferred_element_type=jnp.float32)
            acc[h] = acc[h] * ratio + update

        ahead = score(0)
        held = None
        for h in range(heads):
            scores = ahead
            if h + 1 < heads:
                ahead = score(h + 1)
            old = top[h : h + 1, :]
            new = jnp.maximum(old, jnp.max(scores, axis=0, keepdims=True))
            weights = jnp.exp2((scores - new) * EXP_SCALE)
            ratio = jnp.exp2((old - new) * EXP_SCALE)
            total[h : h + 1, :] = total[h : h + 1, :] * ratio + jnp.sum(
                weights, axis=0, keepdims=True
            )
            top[h : h + 1, :] = new
            if held is not None:
                absorb(*held)
            held = (h, weights.astype(jnp.bfloat16), ratio)
        absorb(*held)

    def own(i, _):
        attend(0, 2 * i, 0, 2 * i + 1)
        return 0

    lax.fori_loop(0, CHUNKS // 2, own, 0)

    pl.semaphore_wait(met.at[0], round_one)
    two_hops = [*along("seq_1", nz, iz, (2, -2)), *along("seq_0", nx, ix, range(1, nx))]
    round_two = greet(met.at[1], two_hops)

    def neighbour(i, _):
        arrived(1, 2 * i)
        arrived(1, 2 * i + 1)
        attend(1, 2 * i, 1, 2 * i + 1)
        return 0

    lax.fori_loop(0, jnp.where(ic == 1, CHUNKS // 2, 0), neighbour, 0)

    pl.semaphore_wait(met.at[1], round_two)
    round_three = greet(met.at[2], [partner])

    mixed = jnp.where(ic == 0, 1, 3)

    def middle(c, _):
        arrived(2, c)
        hand_on(1, 2, c, 4, next_chip).start()
        hand_on(3, 2, c, 4 - mixed, partner).start()
        arrived(mixed, c)
        attend(2, c, mixed, c)
        return 0

    lax.fori_loop(0, CHUNKS, middle, 0)
    pl.semaphore_wait(met.at[2], round_three)

    @pl.when(ic == 0)
    def _():
        def far(c, _):
            arrived(4, c)
            arrived(3, c)
            attend(4, c, 3, c)
            return 0

        lax.fori_loop(0, CHUNKS, far, 0)

    @pl.when(ic == 1)
    def _():
        def far(i, _):
            for c in (2 * i, 2 * i + 1):
                arrived(4, c)
                hand_on(4, 4, c, 3, partner).start()
            attend(4, 2 * i, 4, 2 * i + 1)
            return 0

        lax.fori_loop(0, CHUNKS // 2, far, 0)

    marks = mark_ref[...].astype(jnp.float32)
    squares = jnp.zeros((1, rows), jnp.float32)
    for h in range(heads):
        total[h : h + 1, :] = 1.0 / total[h : h + 1, :]
        attended = acc[h] * total[h : h + 1, :]
        squares = squares + jnp.sum(attended * attended, axis=0, keepdims=True)

    def folded(row):
        return sum(row[:, i : i + 128] for i in range(0, rows, 128))

    part = jnp.concatenate([folded(marks * squares), folded(marks)], 0)
    sent = []
    for stage, (plane, parts) in enumerate(zip(planes, (parts_a, parts_b), strict=True)):
        here = plane[0][2] * plane[1][1] + plane[1][2]

        def partial_copy(d, slot, peer):
            return pltpu.make_async_remote_copy(
                src_ref=parts.at[here],
                dst_ref=parts.at[slot],
                send_sem=part_send.at[stage, d],
                recv_sem=part_recv.at[stage, slot],
                device_id=peer,
                device_id_type=MESH,
            )

        parts[here] = part
        copies = [partial_copy(d, here, peer) for d, _, peer in others(plane)]
        for copy in copies:
            copy.start()
        if stage == 0:
            for h in range(heads):
                attended = acc[h] * total[h : h + 1, :]
                out_vm[:, h * HEAD_WIDTH : (h + 1) * HEAD_WIDTH] = attended.astype(jnp.bfloat16).T
            store = pltpu.make_async_copy(out_vm, out_hbm, store_sem)
            store.start()
        for d, slot, peer in others(plane):
            partial_copy(d, slot, peer).wait_recv()
        part = parts[0]
        for i in range(1, plane[0][1] * plane[1][1]):
            part = part + parts[i]
        sent += copies
    objective = jnp.sum(part[0:1, :]) / ((QUERY_HEADS // nh) * jnp.sum(part[1:2, :]))
    obj_ref[0, 0] = objective

    for copy in sent:
        copy.wait_send()
    for c in range(CHUNKS):
        hand_on(0, 0, c, 2, next_chip).wait_send()
        hand_on(1, 2, c, 4, next_chip).wait_send()
        hand_on(3, 2, c, 4 - mixed, partner).wait_send()

    @pl.when(ic == 0)
    def _():
        for c in range(CHUNKS):
            hand_on(2, 0, c, 1, partner).wait_send()

    @pl.when(ic == 1)
    def _():
        for c in range(CHUNKS):
            hand_on(4, 4, c, 3, partner).wait_send()

    store.wait()


def on_device(sizes, queries, keys, values, doc_start, hop_counts, loss_mask):
    nx, nz, nc, nh = sizes
    rows, width = queries.shape
    kv_width = keys.shape[1]
    heads = width // HEAD_WIDTH
    most = max(nz * nc, nh * nx)
    attention, objective = pl.pallas_call(
        functools.partial(kernel, sizes),
        out_shape=(
            jax.ShapeDtypeStruct((rows, width), jnp.bfloat16),
            jax.ShapeDtypeStruct((1, 1), jnp.float32),
        ),
        in_specs=[pl.BlockSpec(memory_space=pltpu.HBM)] * 6,
        out_specs=(
            pl.BlockSpec(memory_space=pltpu.HBM),
            pl.BlockSpec(memory_space=pltpu.SMEM),
        ),
        scratch_shapes=[
            pltpu.VMEM((HOPS + 1, 2, rows, kv_width), jnp.bfloat16),
            pltpu.VMEM((1, rows), jnp.int32),
            pltpu.SMEM((1,), jnp.int32),
            pltpu.VMEM((1, rows), jnp.int32),
            pltpu.VMEM((rows, width), jnp.bfloat16),
            pltpu.VMEM((heads, HEAD_WIDTH, rows), jnp.bfloat16),
            pltpu.VMEM((heads, HEAD_WIDTH, rows), jnp.float32),
            pltpu.VMEM((heads, rows), jnp.float32),
            pltpu.VMEM((heads, rows), jnp.float32),
            pltpu.VMEM((2 * rows // CHUNKS, rows), jnp.float32),
            pltpu.VMEM((rows, width), jnp.bfloat16),
            pltpu.VMEM((nz * nc, 2, 128), jnp.float32),
            pltpu.VMEM((nh * nx, 2, 128), jnp.float32),
            pltpu.SemaphoreType.DMA((6,)),
            pltpu.SemaphoreType.DMA,
            pltpu.SemaphoreType.DMA((5, CHUNKS)),
            pltpu.SemaphoreType.DMA((HOPS + 1, CHUNKS)),
            pltpu.SemaphoreType.DMA((2, most)),
            pltpu.SemaphoreType.DMA((2, most)),
            pltpu.SemaphoreType.REGULAR((3,)),
        ],
        compiler_params=pltpu.CompilerParams(collective_id=0,
            has_side_effects=True,
        ),
    )(
        queries,
        keys,
        values,
        doc_start.reshape(1, rows),
        hop_counts,
        loss_mask.reshape(1, rows),
    )
    return attention, objective.reshape(())


def solution(mesh):
    nh = mesh.shape["head"]
    devices = mesh.devices.reshape(4, 8, 2, nh)
    torus = Mesh(devices, (*SEQ, "head"))
    placed = (P(SEQ, "head"), P(SEQ, "head"), P(SEQ, "head"), P(SEQ), P(SEQ), P(SEQ))
    return jax.shard_map(
        functools.partial(on_device, devices.shape),
        mesh=torus,
        in_specs=placed,
        out_specs=(P(SEQ, "head"), P()),
        check_vma=False,
    )
```

```python
import functools
import math

import jax
import jax.numpy as jnp
from jax import lax
from jax.experimental import pallas as pl
from jax.experimental.pallas import tpu as pltpu
from jax.sharding import Mesh
from jax.sharding import PartitionSpec as P

QUERY_HEADS = 32
KEY_VALUE_HEADS = 8
HEAD_WIDTH = 128
HOPS = 4
GROUP = QUERY_HEADS // KEY_VALUE_HEADS
CHUNKS = 4
SEQ = ("seq_0", "seq_1", "seq_2")
MESH = pl.DeviceIdType.MESH
EXP_SCALE = math.log2(math.e) / math.sqrt(HEAD_WIDTH)
HIDDEN = -1e30


def kernel(
    sizes,
    q_hbm,
    k_hbm,
    v_hbm,
    doc_hbm,
    hop_hbm,
    mark_hbm,
    out_vm,
    obj_ref,
    kv,
    doc_ref,
    hop_ref,
    mark_ref,
    q_in,
    q_t,
    acc,
    top,
    total,
    bias,
    parts_a,
    parts_b,
    load_sem,
    send_sem,
    recv_sem,
    part_send,
    part_recv,
    met,
):
    nx, nz, nc, nh = sizes
    rows = q_in.shape[0]
    kv_heads = kv.shape[3] // HEAD_WIDTH
    heads = kv_heads * GROUP
    step_rows = rows // CHUNKS
    ix, iz, ic, ih = (lax.axis_index(a) for a in (*SEQ, "head"))
    chip = ix * nz + iz
    block = chip * nc + ic
    after = lax.rem(chip + 1, nx * nz)
    before = lax.rem(chip + nx * nz - 1, nx * nz)
    next_chip = {"seq_0": after // nz, "seq_1": lax.rem(after, nz)}
    last_chip = {"seq_0": before // nz, "seq_1": lax.rem(before, nz)}
    partner = {"seq_2": 1 - ic}
    planes = (
        (("seq_1", nz, iz), ("seq_2", nc, ic)),
        (("head", nh, ih), ("seq_0", nx, ix)),
    )

    def others(plane):
        (name_a, size_a, here_a), (name_b, size_b, here_b) = plane
        for d in range(1, size_a * size_b):
            at_a = lax.rem(here_a + d // size_b, size_a)
            at_b = lax.rem(here_b + d % size_b, size_b)
            yield d, at_a * size_b + at_b, {name_a: at_a, name_b: at_b}

    loads = (
        pltpu.make_async_copy(k_hbm, kv.at[0, 0], load_sem.at[0]),
        pltpu.make_async_copy(v_hbm, kv.at[0, 1], load_sem.at[1]),
        pltpu.make_async_copy(q_hbm, q_in, load_sem.at[2]),
        pltpu.make_async_copy(doc_hbm, doc_ref, load_sem.at[3]),
        pltpu.make_async_copy(hop_hbm, hop_ref, load_sem.at[4]),
        pltpu.make_async_copy(mark_hbm, mark_ref, load_sem.at[5]),
    )
    for load in loads:
        load.start()

    def along(name, size, here, steps):
        return [{name: lax.rem(here + d, size)} for d in sorted({s % size for s in steps} - {0})]

    def greet(semaphore, devices):
        for device in devices:
            pl.semaphore_signal(semaphore, inc=1, device_id=device, device_id_type=MESH)
        return len(devices)

    one_hop = [
        *along("seq_1", nz, iz, (1, -1)),
        *along("seq_0", nx, ix, (1, -1)),
        *along("head", nh, ih, (1, -1)),
    ]
    barrier = pltpu.get_barrier_semaphore()
    signals = greet(barrier, [next_chip, last_chip, partner, *one_hop])
    loads[0].wait()
    loads[1].wait()
    pl.semaphore_wait(barrier, signals)

    def piece(slot, c):
        return kv.at[slot, :, pl.ds(pl.multiple_of(c * step_rows, step_rows), step_rows), :]

    def hand_on(kind, slot, c, to_slot, device):
        return pltpu.make_async_remote_copy(
            src_ref=piece(slot, c),
            dst_ref=piece(to_slot, c),
            send_sem=send_sem.at[kind, c],
            recv_sem=recv_sem.at[to_slot, c],
            device_id=device,
            device_id_type=MESH,
        )

    def arrived(slot, c):
        hand_on(0, 0, c, slot, next_chip).wait_recv()

    for c in range(CHUNKS):
        hand_on(0, 0, c, 2, next_chip).start()

    @pl.when(ic == 0)
    def _():
        for c in range(CHUNKS):
            hand_on(2, 0, c, 1, partner).start()

    round_one = greet(met.at[0], one_hop)
    for load in loads[2:]:
        load.wait()
    for h in range(heads):
        q_t[h] = q_in[:, h * HEAD_WIDTH : (h + 1) * HEAD_WIDTH].T
    top[...] = jnp.full(top.shape, HIDDEN, jnp.float32)
    total[...] = jnp.zeros(total.shape, jnp.float32)
    acc[...] = jnp.zeros(acc.shape, jnp.float32)

    first_key = jnp.maximum(doc_ref[...], (block - hop_ref[0]) * rows)
    q_place = block * rows + lax.broadcasted_iota(jnp.int32, (1, rows), 1)

    def attend(slot_a, c_a, slot_b, c_b, width):
        at_a = pl.ds(pl.multiple_of(c_a * step_rows, step_rows), step_rows)
        at_b = pl.ds(pl.multiple_of(c_b * step_rows, step_rows), step_rows)
        inside = lax.broadcasted_iota(jnp.int32, (step_rows, width), 0)
        for i, (slot, c) in enumerate(((slot_a, c_a), (slot_b, c_b))):
            place = inside + ((block - slot) * rows + c * step_rows)
            seen = (place >= first_key[:, :width]) & (place <= q_place[:, :width])
            bias[i * step_rows : (i + 1) * step_rows, :width] = jnp.where(seen, 0.0, HIDDEN)
        k_two, v_t = [], []
        for g in range(kv_heads):
            lanes = slice(g * HEAD_WIDTH, (g + 1) * HEAD_WIDTH)
            k_two.append(jnp.concatenate([kv[slot_a, 0, at_a, lanes], kv[slot_b, 0, at_b, lanes]], 0))
            v_two = jnp.concatenate([kv[slot_a, 1, at_a, lanes], kv[slot_b, 1, at_b, lanes]], 0)
            v_t.append(v_two.T)

        def score(h):
            raw = jnp.dot(
                k_two[h // GROUP], q_t[h, :, :width], preferred_element_type=jnp.float32
            )
            return raw + bias[:, :width]

        def absorb(h, rounded, ratio):
            update = jnp.dot(v_t[h // GROUP], rounded, preferred_element_type=jnp.float32)
            acc[h, :, :width] = acc[h, :, :width] * ratio + update

        ahead = score(0)
        held = None
        for h in range(heads):
            scores = ahead
            if h + 1 < heads:
                ahead = score(h + 1)
            row = slice(h, h + 1)
            old = top[row, :width]
            new = jnp.maximum(old, jnp.max(scores, axis=0, keepdims=True))
            weights = jnp.exp2((scores - new) * EXP_SCALE)
            ratio = jnp.exp2((old - new) * EXP_SCALE)
            total[row, :width] = total[row, :width] * ratio + jnp.sum(
                weights, axis=0, keepdims=True
            )
            top[row, :width] = new
            if held is not None:
                absorb(*held)
            held = (h, weights.astype(jnp.bfloat16), ratio)
        absorb(*held)

    def own(i, _):
        attend(0, 2 * i, 0, 2 * i + 1, rows)
        return 0

    lax.fori_loop(0, CHUNKS // 2, own, 0)

    pl.semaphore_wait(met.at[0], round_one)
    two_hops = [*along("seq_1", nz, iz, (2, -2)), *along("seq_0", nx, ix, range(1, nx))]
    round_two = greet(met.at[1], two_hops)

    def neighbour(i, _):
        arrived(1, 2 * i)
        arrived(1, 2 * i + 1)
        attend(1, 2 * i, 1, 2 * i + 1, rows)
        return 0

    lax.fori_loop(0, jnp.where(ic == 1, CHUNKS // 2, 0), neighbour, 0)

    pl.semaphore_wait(met.at[1], round_two)
    round_three = greet(met.at[2], [partner])

    mixed = jnp.where(ic == 0, 1, 3)

    def middle(c, _):
        arrived(2, c)
        hand_on(3, 2, c, 4 - mixed, partner).start()

        @pl.when(ic == 1)
        def _():
            hand_on(1, 2, c, 4, next_chip).start()

        @pl.when((ic == 0) & (c == CHUNKS - 1))
        def _():
            for late in range(CHUNKS - 1, -1, -1):
                hand_on(1, 2, late, 4, next_chip).start()

        arrived(mixed, c)
        attend(2, c, mixed, c, rows)
        return 0

    lax.fori_loop(0, CHUNKS, middle, 0)
    pl.semaphore_wait(met.at[2], round_three)

    @pl.when(ic == 0)
    def _():
        def far(i, _):
            later = jnp.minimum(i, 1)
            c_a = i + later
            slot_b = 3 + later
            c_b = jnp.where(i == 0, 1, CHUNKS - i)
            arrived(3, c_a)
            arrived(slot_b, c_b)
            attend(3, c_a, slot_b, c_b, rows)
            return 0

        lax.fori_loop(0, CHUNKS - 1, far, 0)
        arrived(4, 1)
        arrived(4, 0)
        attend(4, 1, 4, 0, rows // 2)

    @pl.when(ic == 1)
    def _():
        def far(i, _):
            for c in (2 * i, 2 * i + 1):
                arrived(4, c)
                hand_on(4, 4, c, 3, partner).start()
            attend(4, 2 * i, 4, 2 * i + 1, rows)
            return 0

        lax.fori_loop(0, CHUNKS // 2, far, 0)

    marks = mark_ref[...].astype(jnp.float32)
    squares = jnp.zeros((1, rows), jnp.float32)
    for h in range(heads):
        total[h : h + 1, :] = 1.0 / total[h : h + 1, :]
        attended = acc[h] * total[h : h + 1, :]
        squares = squares + jnp.sum(attended * attended, axis=0, keepdims=True)

    def folded(row):
        return sum(row[:, i : i + 128] for i in range(0, rows, 128))

    part = jnp.concatenate([folded(marks * squares), folded(marks)], 0)
    sent = []
    for stage, (plane, parts) in enumerate(zip(planes, (parts_a, parts_b), strict=True)):
        here = plane[0][2] * plane[1][1] + plane[1][2]

        def partial_copy(d, slot, peer):
            return pltpu.make_async_remote_copy(
                src_ref=parts.at[here],
                dst_ref=parts.at[slot],
                send_sem=part_send.at[stage, d],
                recv_sem=part_recv.at[stage, slot],
                device_id=peer,
                device_id_type=MESH,
            )

        parts[here] = part
        copies = [partial_copy(d, here, peer) for d, _, peer in others(plane)]
        for copy in copies:
            copy.start()
        if stage == 0:
            for h in range(heads):
                attended = acc[h] * total[h : h + 1, :]
                out_vm[:, h * HEAD_WIDTH : (h + 1) * HEAD_WIDTH] = attended.astype(jnp.bfloat16).T
        for d, slot, peer in others(plane):
            partial_copy(d, slot, peer).wait_recv()
        part = parts[0]
        for i in range(1, plane[0][1] * plane[1][1]):
            part = part + parts[i]
        sent += copies
    objective = jnp.sum(part[0:1, :]) / ((QUERY_HEADS // nh) * jnp.sum(part[1:2, :]))
    obj_ref[0, 0] = objective

    for copy in sent:
        copy.wait_send()
    for c in range(CHUNKS):
        hand_on(0, 0, c, 2, next_chip).wait_send()
        hand_on(1, 2, c, 4, next_chip).wait_send()
        hand_on(3, 2, c, 4 - mixed, partner).wait_send()

    @pl.when(ic == 0)
    def _():
        for c in range(CHUNKS):
            hand_on(2, 0, c, 1, partner).wait_send()

    @pl.when(ic == 1)
    def _():
        for c in range(CHUNKS):
            hand_on(4, 4, c, 3, partner).wait_send()


def in_hbm(array):
    return pltpu.with_memory_space_constraint(array, pltpu.HBM)


def on_device(sizes, queries, keys, values, doc_start, hop_counts, loss_mask):
    nx, nz, nc, nh = sizes
    rows, width = queries.shape
    kv_width = keys.shape[1]
    heads = width // HEAD_WIDTH
    most = max(nz * nc, nh * nx)
    attention, objective = pl.pallas_call(
        functools.partial(kernel, sizes),
        out_shape=(
            jax.ShapeDtypeStruct((rows, width), jnp.bfloat16),
            jax.ShapeDtypeStruct((1, 1), jnp.float32),
        ),
        in_specs=[pl.BlockSpec(memory_space=pltpu.HBM)] * 6,
        out_specs=(
            pl.BlockSpec(memory_space=pltpu.VMEM),
            pl.BlockSpec(memory_space=pltpu.SMEM),
        ),
        scratch_shapes=[
            pltpu.VMEM((HOPS + 1, 2, rows, kv_width), jnp.bfloat16),
            pltpu.VMEM((1, rows), jnp.int32),
            pltpu.SMEM((1,), jnp.int32),
            pltpu.VMEM((1, rows), jnp.int32),
            pltpu.VMEM((rows, width), jnp.bfloat16),
            pltpu.VMEM((heads, HEAD_WIDTH, rows), jnp.bfloat16),
            pltpu.VMEM((heads, HEAD_WIDTH, rows), jnp.float32),
            pltpu.VMEM((heads, rows), jnp.float32),
            pltpu.VMEM((heads, rows), jnp.float32),
            pltpu.VMEM((2 * rows // CHUNKS, rows), jnp.float32),
            pltpu.VMEM((nz * nc, 2, 128), jnp.float32),
            pltpu.VMEM((nh * nx, 2, 128), jnp.float32),
            pltpu.SemaphoreType.DMA((6,)),
            pltpu.SemaphoreType.DMA((5, CHUNKS)),
            pltpu.SemaphoreType.DMA((HOPS + 1, CHUNKS)),
            pltpu.SemaphoreType.DMA((2, most)),
            pltpu.SemaphoreType.DMA((2, most)),
            pltpu.SemaphoreType.REGULAR((3,)),
        ],
        compiler_params=pltpu.CompilerParams(collective_id=0,
            vmem_limit_bytes=20 * 1024 * 1024,
            has_side_effects=True,
        ),
    )(
        in_hbm(queries),
        in_hbm(keys),
        in_hbm(values),
        in_hbm(doc_start.reshape(1, rows)),
        hop_counts,
        in_hbm(loss_mask.reshape(1, rows)),
    )
    return attention, objective.reshape(())


def solution(mesh):
    nh = mesh.shape["head"]
    devices = mesh.devices.reshape(4, 8, 2, nh)
    torus = Mesh(devices, (*SEQ, "head"))
    placed = (P(SEQ, "head"), P(SEQ, "head"), P(SEQ, "head"), P(SEQ), P(SEQ), P(SEQ))
    return jax.shard_map(
        functools.partial(on_device, devices.shape),
        mesh=torus,
        in_specs=placed,
        out_specs=(P(SEQ, "head"), P()),
        check_vma=False,
    )
```

```python
import functools
import math

import jax
import jax.numpy as jnp
from jax import lax
from jax.experimental import pallas as pl
from jax.experimental.pallas import tpu as pltpu
from jax.sharding import Mesh
from jax.sharding import PartitionSpec as P

QUERY_HEADS = 32
KEY_VALUE_HEADS = 8
HEAD_WIDTH = 128
HOPS = 4
GROUP = QUERY_HEADS // KEY_VALUE_HEADS
CHUNKS = 4
SEQ = ("seq_0", "seq_1", "seq_2")
MESH = pl.DeviceIdType.MESH
EXP_SCALE = math.log2(math.e) / math.sqrt(HEAD_WIDTH)
HIDDEN = -1e30


def kernel(
    sizes,
    q_hbm,
    k_hbm,
    v_hbm,
    doc_hbm,
    hop_hbm,
    mark_hbm,
    out_vm,
    obj_ref,
    kv,
    doc_ref,
    hop_ref,
    mark_ref,
    q_in,
    q_t,
    acc,
    top,
    total,
    bias,
    parts_a,
    parts_b,
    load_sem,
    send_sem,
    recv_sem,
    part_send,
    part_recv,
    met,
):
    nx, nz, nc, nh = sizes
    rows = q_in.shape[0]
    kv_heads = kv.shape[3] // HEAD_WIDTH
    heads = kv_heads * GROUP
    step_rows = rows // CHUNKS
    ix, iz, ic, ih = (lax.axis_index(a) for a in (*SEQ, "head"))
    chip = ix * nz + iz
    block = chip * nc + ic
    after = lax.rem(chip + 1, nx * nz)
    before = lax.rem(chip + nx * nz - 1, nx * nz)
    next_chip = {"seq_0": after // nz, "seq_1": lax.rem(after, nz)}
    last_chip = {"seq_0": before // nz, "seq_1": lax.rem(before, nz)}
    partner = {"seq_2": 1 - ic}
    planes = (
        (("seq_1", nz, iz), ("seq_2", nc, ic)),
        (("head", nh, ih), ("seq_0", nx, ix)),
    )

    def others(plane):
        (name_a, size_a, here_a), (name_b, size_b, here_b) = plane
        for d in range(1, size_a * size_b):
            at_a = lax.rem(here_a + d // size_b, size_a)
            at_b = lax.rem(here_b + d % size_b, size_b)
            yield d, at_a * size_b + at_b, {name_a: at_a, name_b: at_b}

    loads = (
        pltpu.make_async_copy(k_hbm, kv.at[0, 0], load_sem.at[0]),
        pltpu.make_async_copy(v_hbm, kv.at[0, 1], load_sem.at[1]),
        pltpu.make_async_copy(q_hbm, q_in, load_sem.at[2]),
        pltpu.make_async_copy(doc_hbm, doc_ref, load_sem.at[3]),
        pltpu.make_async_copy(hop_hbm, hop_ref, load_sem.at[4]),
        pltpu.make_async_copy(mark_hbm, mark_ref, load_sem.at[5]),
    )
    for load in loads:
        load.start()

    def along(name, size, here, steps):
        return [{name: lax.rem(here + d, size)} for d in sorted({s % size for s in steps} - {0})]

    def greet(semaphore, devices):
        for device in devices:
            pl.semaphore_signal(semaphore, inc=1, device_id=device, device_id_type=MESH)
        return len(devices)

    one_hop = [
        *along("seq_1", nz, iz, (1, -1)),
        *along("seq_0", nx, ix, (1, -1)),
        *along("head", nh, ih, (1, -1)),
    ]
    barrier = pltpu.get_barrier_semaphore()
    signals = greet(barrier, [next_chip, last_chip, partner, *one_hop])
    loads[0].wait()
    loads[1].wait()
    pl.semaphore_wait(barrier, signals)

    def piece(slot, c):
        return kv.at[slot, :, pl.ds(pl.multiple_of(c * step_rows, step_rows), step_rows), :]

    def hand_on(kind, slot, c, to_slot, device):
        return pltpu.make_async_remote_copy(
            src_ref=piece(slot, c),
            dst_ref=piece(to_slot, c),
            send_sem=send_sem.at[kind, c],
            recv_sem=recv_sem.at[to_slot, c],
            device_id=device,
            device_id_type=MESH,
        )

    def arrived(slot, c):
        hand_on(0, 0, c, slot, next_chip).wait_recv()

    for c in range(CHUNKS):
        hand_on(0, 0, c, 2, next_chip).start()

    @pl.when(ic == 0)
    def _():
        for c in range(CHUNKS):
            hand_on(2, 0, c, 1, partner).start()

    round_one = greet(met.at[0], one_hop)
    for load in loads[2:]:
        load.wait()
    for h in range(heads):
        q_t[h] = q_in[:, h * HEAD_WIDTH : (h + 1) * HEAD_WIDTH].T
    top[...] = jnp.full(top.shape, HIDDEN, jnp.float32)
    total[...] = jnp.zeros(total.shape, jnp.float32)
    acc[...] = jnp.zeros(acc.shape, jnp.float32)

    first_key = jnp.maximum(doc_ref[...], (block - hop_ref[0]) * rows)
    q_place = block * rows + lax.broadcasted_iota(jnp.int32, (1, rows), 1)

    def attend(slot_a, c_a, slot_b, c_b, width):
        at_a = pl.ds(pl.multiple_of(c_a * step_rows, step_rows), step_rows)
        at_b = pl.ds(pl.multiple_of(c_b * step_rows, step_rows), step_rows)
        inside = lax.broadcasted_iota(jnp.int32, (step_rows, width), 0)
        for i, (slot, c) in enumerate(((slot_a, c_a), (slot_b, c_b))):
            place = inside + ((block - slot) * rows + c * step_rows)
            seen = (place >= first_key[:, :width]) & (place <= q_place[:, :width])
            bias[i * step_rows : (i + 1) * step_rows, :width] = jnp.where(seen, 0.0, HIDDEN)
        k_two, v_t = [], []
        for g in range(kv_heads):
            lanes = slice(g * HEAD_WIDTH, (g + 1) * HEAD_WIDTH)
            k_two.append(jnp.concatenate([kv[slot_a, 0, at_a, lanes], kv[slot_b, 0, at_b, lanes]], 0))
            v_two = jnp.concatenate([kv[slot_a, 1, at_a, lanes], kv[slot_b, 1, at_b, lanes]], 0)
            v_t.append(v_two.T)

        def score(h):
            raw = jnp.dot(
                k_two[h // GROUP], q_t[h, :, :width], preferred_element_type=jnp.float32
            )
            return raw + bias[:, :width]

        def absorb(h, rounded, ratio):
            update = jnp.dot(v_t[h // GROUP], rounded, preferred_element_type=jnp.float32)
            acc[h, :, :width] = acc[h, :, :width] * ratio + update

        ahead = score(0)
        held = None
        for h in range(heads):
            scores = ahead
            if h + 1 < heads:
                ahead = score(h + 1)
            row = slice(h, h + 1)
            old = top[row, :width]
            new = jnp.maximum(old, jnp.max(scores, axis=0, keepdims=True))
            weights = jnp.exp2((scores - new) * EXP_SCALE)
            ratio = jnp.exp2((old - new) * EXP_SCALE)
            total[row, :width] = total[row, :width] * ratio + jnp.sum(
                weights, axis=0, keepdims=True
            )
            top[row, :width] = new
            if held is not None:
                absorb(*held)
            held = (h, weights.astype(jnp.bfloat16), ratio)
        absorb(*held)

    def own(i, _):
        attend(0, 2 * i, 0, 2 * i + 1, rows)
        return 0

    lax.fori_loop(0, CHUNKS // 2, own, 0)

    pl.semaphore_wait(met.at[0], round_one)
    two_hops = [*along("seq_1", nz, iz, (2, -2)), *along("seq_0", nx, ix, range(1, nx))]
    round_two = greet(met.at[1], two_hops)

    def neighbour(i, _):
        arrived(1, 2 * i)
        arrived(1, 2 * i + 1)
        attend(1, 2 * i, 1, 2 * i + 1, rows)
        return 0

    lax.fori_loop(0, jnp.where(ic == 1, CHUNKS // 2, 0), neighbour, 0)

    pl.semaphore_wait(met.at[1], round_two)
    round_three = greet(met.at[2], [partner])

    mixed = jnp.where(ic == 0, 1, 3)

    def middle(c, _):
        arrived(2, c)
        hand_on(3, 2, c, 4 - mixed, partner).start()

        @pl.when(ic == 1)
        def _():
            hand_on(1, 2, c, 4, next_chip).start()

        @pl.when((ic == 0) & (c == CHUNKS - 1))
        def _():
            for late in range(CHUNKS - 1, -1, -1):
                hand_on(1, 2, late, 4, next_chip).start()

        arrived(mixed, c)
        attend(2, c, mixed, c, rows)
        return 0

    lax.fori_loop(0, CHUNKS, middle, 0)
    pl.semaphore_wait(met.at[2], round_three)

    @pl.when(ic == 0)
    def _():
        def far(i, _):
            later = jnp.minimum(i, 1)
            c_a = i + later
            slot_b = 3 + later
            c_b = jnp.where(i == 0, 1, CHUNKS - i)
            arrived(3, c_a)
            arrived(slot_b, c_b)
            attend(3, c_a, slot_b, c_b, rows)
            return 0

        lax.fori_loop(0, CHUNKS - 1, far, 0)
        arrived(4, 1)
        arrived(4, 0)
        attend(4, 1, 4, 0, rows // 2)

    @pl.when(ic == 1)
    def _():
        for first, width in ((0, rows // 2), (2, rows)):
            for c in (first, first + 1):
                arrived(4, c)
                hand_on(4, 4, c, 3, partner).start()
            attend(4, first, 4, first + 1, width)

    marks = mark_ref[...].astype(jnp.float32)
    squares = jnp.zeros((1, rows), jnp.float32)
    for h in range(heads):
        total[h : h + 1, :] = 1.0 / total[h : h + 1, :]
        attended = acc[h] * total[h : h + 1, :]
        squares = squares + jnp.sum(attended * attended, axis=0, keepdims=True)

    def folded(row):
        return sum(row[:, i : i + 128] for i in range(0, rows, 128))

    part = jnp.concatenate([folded(marks * squares), folded(marks)], 0)
    sent = []
    for stage, (plane, parts) in enumerate(zip(planes, (parts_a, parts_b), strict=True)):
        here = plane[0][2] * plane[1][1] + plane[1][2]

        def partial_copy(d, slot, peer):
            return pltpu.make_async_remote_copy(
                src_ref=parts.at[here],
                dst_ref=parts.at[slot],
                send_sem=part_send.at[stage, d],
                recv_sem=part_recv.at[stage, slot],
                device_id=peer,
                device_id_type=MESH,
            )

        parts[here] = part
        copies = [partial_copy(d, here, peer) for d, _, peer in others(plane)]
        for copy in copies:
            copy.start()
        if stage == 0:
            for h in range(heads):
                attended = acc[h] * total[h : h + 1, :]
                out_vm[:, h * HEAD_WIDTH : (h + 1) * HEAD_WIDTH] = attended.astype(jnp.bfloat16).T
        for d, slot, peer in others(plane):
            partial_copy(d, slot, peer).wait_recv()
        part = parts[0]
        for i in range(1, plane[0][1] * plane[1][1]):
            part = part + parts[i]
        sent += copies
    objective = jnp.sum(part[0:1, :]) / ((QUERY_HEADS // nh) * jnp.sum(part[1:2, :]))
    obj_ref[0, 0] = objective

    for copy in sent:
        copy.wait_send()
    for c in range(CHUNKS):
        hand_on(0, 0, c, 2, next_chip).wait_send()
        hand_on(1, 2, c, 4, next_chip).wait_send()
        hand_on(3, 2, c, 4 - mixed, partner).wait_send()

    @pl.when(ic == 0)
    def _():
        for c in range(CHUNKS):
            hand_on(2, 0, c, 1, partner).wait_send()

    @pl.when(ic == 1)
    def _():
        for c in range(CHUNKS):
            hand_on(4, 4, c, 3, partner).wait_send()


def in_hbm(array):
    return pltpu.with_memory_space_constraint(array, pltpu.HBM)


def on_device(sizes, queries, keys, values, doc_start, hop_counts, loss_mask):
    nx, nz, nc, nh = sizes
    rows, width = queries.shape
    kv_width = keys.shape[1]
    heads = width // HEAD_WIDTH
    most = max(nz * nc, nh * nx)
    attention, objective = pl.pallas_call(
        functools.partial(kernel, sizes),
        out_shape=(
            jax.ShapeDtypeStruct((rows, width), jnp.bfloat16),
            jax.ShapeDtypeStruct((1, 1), jnp.float32),
        ),
        in_specs=[pl.BlockSpec(memory_space=pltpu.HBM)] * 6,
        out_specs=(
            pl.BlockSpec(memory_space=pltpu.VMEM),
            pl.BlockSpec(memory_space=pltpu.SMEM),
        ),
        scratch_shapes=[
            pltpu.VMEM((HOPS + 1, 2, rows, kv_width), jnp.bfloat16),
            pltpu.VMEM((1, rows), jnp.int32),
            pltpu.SMEM((1,), jnp.int32),
            pltpu.VMEM((1, rows), jnp.int32),
            pltpu.VMEM((rows, width), jnp.bfloat16),
            pltpu.VMEM((heads, HEAD_WIDTH, rows), jnp.bfloat16),
            pltpu.VMEM((heads, HEAD_WIDTH, rows), jnp.float32),
            pltpu.VMEM((heads, rows), jnp.float32),
            pltpu.VMEM((heads, rows), jnp.float32),
            pltpu.VMEM((2 * rows // CHUNKS, rows), jnp.float32),
            pltpu.VMEM((nz * nc, 2, 128), jnp.float32),
            pltpu.VMEM((nh * nx, 2, 128), jnp.float32),
            pltpu.SemaphoreType.DMA((6,)),
            pltpu.SemaphoreType.DMA((5, CHUNKS)),
            pltpu.SemaphoreType.DMA((HOPS + 1, CHUNKS)),
            pltpu.SemaphoreType.DMA((2, most)),
            pltpu.SemaphoreType.DMA((2, most)),
            pltpu.SemaphoreType.REGULAR((3,)),
        ],
        compiler_params=pltpu.CompilerParams(collective_id=0,
            vmem_limit_bytes=20 * 1024 * 1024,
            has_side_effects=True,
        ),
    )(
        in_hbm(queries),
        in_hbm(keys),
        in_hbm(values),
        in_hbm(doc_start.reshape(1, rows)),
        hop_counts,
        in_hbm(loss_mask.reshape(1, rows)),
    )
    return attention, objective.reshape(())


def solution(mesh):
    nh = mesh.shape["head"]
    devices = mesh.devices.reshape(4, 8, 2, nh)
    torus = Mesh(devices, (*SEQ, "head"))
    placed = (P(SEQ, "head"), P(SEQ, "head"), P(SEQ, "head"), P(SEQ), P(SEQ), P(SEQ))
    return jax.shard_map(
        functools.partial(on_device, devices.shape),
        mesh=torus,
        in_specs=placed,
        out_specs=(P(SEQ, "head"), P()),
        check_vma=False,
    )
```
